16 devices in a mesh: dp: 4 (over z, y), tp: 4 (over x, core).
Axes of the slice: x: 2, y: 2, z: 2, core: 2. Of those that a mesh axis runs over, the one named last changes fastest.
Arguments:
- token_ids: int32 [4, 1024], P('dp'), parts along dimension 0
- emb_table: bfloat16 [32000, 2048], P('tp')
- norm_gain: bfloat16 [2048], replicated
- grad_out: bfloat16 [4, 1024, 2048], P('dp', 'tp'), parts along dimension 0
Outputs:
- output 1: bfloat16 [4, 1024, 2048], P('dp', 'tp'), parts along dimension 0
- output 2: float32 [128000, 2048], P(('dp', 'tp')), parts along dimension 0
- output 3: float32 [8192], P('dp'), parts along dimension 0
There are 4 independent parts. The reference program is written for one: setup_inputs(seed, part) draws one part's arguments, and reference() takes and returns one part's arrays. A program takes and returns all parts, laid end to end along the dimension named above; an argument that names none is the same for every part.
All inputs are finite; a program needn't handle non-finite values.
Results may differ from the reference program's by a relative error of at most 0.00852867.
Values are sent between devices in bfloat16 or wider.
A program may use at most 1 GiB of HBM per device.

```python
import jax
import jax.numpy as jnp
from jax import lax

VOCAB_SIZE = 32000
HIDDEN = 2048
BATCH_ROWS = 1
SEQ_LEN = 1024
RMS_EPS = 1e-5


def setup_inputs(seed: int = 0, part: int = 0) -> dict:
    base_key = jax.random.key(seed)
    key_table, key_gain, key_perm, key_ids, key_grad = jax.random.split(base_key, 5)
    popularity = jax.random.permutation(key_perm, VOCAB_SIZE)
    uniform_draws = jax.random.randint(jax.random.fold_in(key_ids, part), (BATCH_ROWS, SEQ_LEN), 1, 1048577)
    ranks = (67108864 // uniform_draws - 64) % VOCAB_SIZE
    token_ids = jnp.take(popularity, ranks).astype(jnp.int32)
    token_ids = token_ids.at[0, 0].set(0).at[BATCH_ROWS - 1, SEQ_LEN - 1].set(VOCAB_SIZE - 1)
    emb_table = jax.random.normal(key_table, (VOCAB_SIZE, HIDDEN), jnp.float32).astype(jnp.bfloat16)
    norm_gain = (1.0 + 0.5 * jax.random.normal(key_gain, (HIDDEN,), jnp.float32)).astype(jnp.bfloat16)
    grad_out = jax.random.normal(jax.random.fold_in(key_grad, part), (BATCH_ROWS, SEQ_LEN, HIDDEN), jnp.float32).astype(jnp.bfloat16)
    return {'token_ids': token_ids, 'emb_table': emb_table, 'norm_gain': norm_gain, 'grad_out': grad_out}


def reference(token_ids, emb_table, norm_gain, grad_out):
    embedded = jnp.take(emb_table, token_ids, axis=0)
    hidden_f32 = embedded.astype(jnp.float32)
    inv_rms = lax.rsqrt(jnp.mean(hidden_f32 * hidden_f32, axis=-1, keepdims=True) + RMS_EPS)
    x_hat = hidden_f32 * inv_rms
    normed = x_hat.astype(jnp.bfloat16) * norm_gain
    grad_f32 = grad_out.astype(jnp.float32)
    grad_gain = jnp.sum(grad_f32 * x_hat, axis=(0, 1))
    grad_hat = grad_f32 * norm_gain.astype(jnp.float32)
    grad_in = inv_rms * (grad_hat - x_hat * jnp.mean(grad_hat * x_hat, axis=-1, keepdims=True))
    grad_rows = grad_in.astype(jnp.bfloat16).astype(jnp.float32).reshape(-1, HIDDEN)
    grad_table = jax.ops.segment_sum(grad_rows, token_ids.reshape(-1), num_segments=VOCAB_SIZE)
    return normed, grad_table, grad_gain
```

```python
import functools

import jax
import jax.numpy as jnp
from jax import lax
from jax.experimental import pallas as pl
from jax.experimental.pallas import tpu as pltpu
from jax.sharding import PartitionSpec as P

RMS_EPS = 1e-5
DY_CAP = 176
X_CAP = 96
U_CAP = 144
DY_SLOT = 192
SLAB = 8
KEY_STEP = 8192.0
NO_KEY = 1.0e6
ACROSS = [(i, i ^ 2) for i in range(4)]
SIBLING = [(i, i ^ 1) for i in range(4)]
F32 = jnp.float32
BF16 = jnp.bfloat16
ANY = pl.BlockSpec(memory_space=pl.ANY)
VMEM = pl.BlockSpec(memory_space=pltpu.VMEM)
SMEM = pl.BlockSpec(memory_space=pltpu.SMEM)


def dot(a, b, ca, cb):
    return lax.dot_general(a, b, (((ca,), (cb,)), ((), ())), preferred_element_type=F32)


def cost(us, moved):
    return pl.CostEstimate(flops=int(us * 2_000_000), bytes_accessed=moved, transcendentals=0)


def iota(shape, axis):
    return lax.broadcasted_iota(jnp.int32, shape, axis)


def owner_of(ids, rows):
    out = jnp.zeros_like(ids)
    for k in (1, 2, 3):
        out += jnp.where(ids >= k * rows, 1, 0)
    return out


def columns(row):
    parts = []
    for j in range(0, row.shape[1], 128):
        parts.append(jnp.broadcast_to(row[:, j:j + 128], (128, 128)).T)
    return jnp.concatenate(parts, axis=0)


def before(n):
    return jnp.where(iota((n, n), 0) < iota((n, n), 1), 1.0, 0.0).astype(BF16)


def pack_kernel(rows, ids_ref, dy_ref, out_ref):
    me = lax.axis_index('tp')
    span = dy_ref.shape[0]
    ids = ids_ref[:, pl.ds(pl.multiple_of(me * span, 128), span)]
    leaves = (owner_of(ids, rows) >= 2) != (me >= 2)
    flag = jnp.broadcast_to(jnp.where(leaves, 1.0, 0.0), (8, span))
    rank = dot(flag.astype(BF16), before(span), 1, 0)[0:1]
    rank = jnp.where(leaves, rank, -1.0)
    slots = iota((DY_CAP, span), 0).astype(F32)
    pick = jnp.where(slots == rank, 1.0, 0.0).astype(BF16)
    out_ref[...] = dot(pick, dy_ref[...], 1, 0).astype(BF16)


def index_kernel(rows, span, ids_ref, idx_ref, lst_ref, flag_ref, rank_ref, src_ref):
    me = lax.axis_index('tp')
    ids = ids_ref[...]
    n = ids.shape[1]
    owner = owner_of(ids, rows)
    local = ids - owner * rows
    pos = iota((1, n), 1)
    idf = ids.astype(F32)
    col = columns(idf)
    posc = iota((n, 128), 0).astype(F32)
    lo, hi = [], []
    for j in range(0, n, 128):
        same = col == idf[:, j:j + 128]
        lo.append(jnp.min(jnp.where(same, posc, 4096.0), axis=0, keepdims=True))
        hi.append(jnp.max(jnp.where(same, posc, -1.0), axis=0, keepdims=True))
    lo = jnp.concatenate(lo, axis=1)
    hi = jnp.concatenate(hi, axis=1)
    first = lo == pos.astype(F32)
    half = n // 2
    wanted = jnp.where(owner < 2, jnp.where(hi >= half, 1.0, 0.0), jnp.where(lo < half, 1.0, 0.0))
    key = (owner.astype(F32) * 2.0 + 1.0 - wanted) * KEY_STEP + local.astype(F32)
    keyf = jnp.where(first, key, NO_KEY)
    kcol = columns(keyf)
    rank = []
    for j in range(0, n, 128):
        rank.append(jnp.sum(jnp.where(kcol < key[:, j:j + 128], 1.0, 0.0), axis=0, keepdims=True))
    rank = jnp.concatenate(rank, axis=1)

    def below(bound):
        return jnp.sum(jnp.where(keyf < bound, 1.0, 0.0), axis=1, keepdims=True)

    base = [below(2.0 * KEY_STEP * o) for o in range(5)]
    over = jnp.zeros((1, 1), F32)
    for o in range(4):
        over = jnp.maximum(over, jnp.where(base[o + 1] - base[o] > U_CAP, 1.0, 0.0))
        over = jnp.maximum(over, jnp.where(below((2.0 * o + 1.0) * KEY_STEP) - base[o] > X_CAP, 1.0, 0.0))
    start = jnp.where(owner == 0, base[0], jnp.where(owner == 1, base[1], jnp.where(owner == 2, base[2], base[3])))
    uidx = rank - start
    mine = owner == me
    uidx_mine = jnp.where(mine, uidx, -1.0)
    idx_ref[0:1, :] = uidx_mine.astype(jnp.int32)

    crosses = (owner >= 2) != (pos >= half)
    flag = jnp.where(crosses, 1.0, 0.0)
    flags = jnp.concatenate([flag[:, h * span:(h + 1) * span] for h in range(4)] + [jnp.zeros((4, span), F32)], axis=0)
    ranks = dot(flags.astype(BF16), before(span), 1, 0)
    over = jnp.maximum(over, jnp.max(jnp.where(jnp.sum(flags, axis=1, keepdims=True) > DY_CAP, 1.0, 0.0), axis=0, keepdims=True))
    rank_ref[...] = jnp.where(flags > 0.5, ranks, -1.0)
    src_ref[0:1, :] = uidx_mine
    rel = owner ^ me
    offset = jnp.where(rel == 0, 0, jnp.where(rel == 1, U_CAP, jnp.where(rel == 2, 2 * U_CAP, 2 * U_CAP + X_CAP)))
    src_ref[1:2, :] = uidx + offset.astype(F32)
    slots = iota((span, span), 0).astype(F32)
    for row, flip in ((2, 2), (3, 3)):
        h = me ^ flip
        there = pl.ds(pl.multiple_of(h * span, 128), span)
        pick = jnp.where(slots == rank_ref[pl.ds(h, 1), :], 1.0, 0.0).astype(BF16)
        value = jnp.broadcast_to(src_ref[0:1, there] + 1.0, (8, span)).astype(BF16)
        idx_ref[row:row + 1, 0:span] = (dot(value, pick, 1, 1)[0:1] - 1.0).astype(jnp.int32)
    idx_ref[1:2, 0:span] = src_ref[1:2, pl.ds(pl.multiple_of(me * span, 128), span)].astype(jnp.int32)

    width = lst_ref.shape[1]
    lead_col = jnp.where(first & mine, uidx, -1.0)
    pick = jnp.where(iota((width, n), 0).astype(F32) == lead_col, 1.0, 0.0).astype(BF16)
    hi8 = local >> 8
    lo8 = local - hi8 * 256
    parts = jnp.concatenate([hi8.astype(F32), lo8.astype(F32), jnp.ones((1, n), F32), jnp.zeros((5, n), F32)], axis=0)
    got = dot(parts.astype(BF16), pick, 1, 1)
    row_of = got[0:1] * 256.0 + got[1:2]
    valid = got[2:3] > 0.5
    slab = jnp.where(valid, jnp.floor(row_of * (1.0 / SLAB)), -1.0)
    scol = columns(slab)
    slotc = iota((width, 128), 0).astype(F32)
    lead = []
    for j in range(0, width, 128):
        lead.append(jnp.min(jnp.where(scol == slab[:, j:j + 128], slotc, 4096.0), axis=0, keepdims=True))
    lead = jnp.concatenate(lead, axis=1)
    lst_ref[0:1, :] = row_of.astype(jnp.int32)
    lst_ref[1:2, :] = lead.astype(jnp.int32)
    count = jnp.sum(jnp.where(valid, 1.0, 0.0), axis=1, keepdims=True)
    lst_ref[2:3, :] = jnp.broadcast_to(jnp.minimum(count, float(U_CAP)), (1, width)).astype(jnp.int32)
    flag_ref[...] = jnp.broadcast_to(over, flag_ref.shape)


def gather_kernel(lst_ref, lrow_ref, table_ref, out_ref, slabs, sem):
    def issue(u, carry):
        pltpu.make_async_copy(table_ref.at[lst_ref[0, u] >> 3], slabs.at[u], sem).start()
        return carry

    lax.fori_loop(0, U_CAP, issue, 0, unroll=8)
    pltpu.make_async_copy(table_ref.at[pl.ds(0, U_CAP)], slabs, sem).wait()
    sub = lrow_ref[0:1, 0:U_CAP] & 7
    want = iota((1, U_CAP), 1) * SLAB + sub
    pick = jnp.where(iota((U_CAP * SLAB, U_CAP), 0) == want, 1.0, 0.0).astype(BF16)
    flat = slabs[...].reshape(U_CAP * SLAB, slabs.shape[2])
    out_ref[...] = dot(pick, flat, 0, 0).astype(BF16)


def dx_kernel(idx_ref, own_ref, sib_ref, got_ref, fwd_ref, u_ref, gain_ref, sum_ref, dg_ref, dy_all, pick_all, sems):
    me = lax.axis_index('tp')
    span = own_ref.shape[0]
    hidden = own_ref.shape[1]
    copies = []
    for k, (src, at) in enumerate(((own_ref, 0), (sib_ref, span), (got_ref, 2 * span), (fwd_ref, 2 * span + DY_SLOT))):
        copies.append(pltpu.make_async_copy(src, dy_all.at[pl.ds(at, src.shape[0])], sems.at[k]))
        copies[-1].start()
    for k in range(2):
        at = 2 * span + k * DY_SLOT
        dy_all[at + DY_CAP:at + DY_SLOT, :] = jnp.zeros((DY_SLOT - DY_CAP, hidden), BF16)
    own_row = idx_ref[0:1, pl.ds(pl.multiple_of(me * span, 128), span)]
    sib_row = idx_ref[0:1, pl.ds(pl.multiple_of((me ^ 1) * span, 128), span)]
    where_row = jnp.concatenate([own_row, sib_row, idx_ref[2:3, 0:DY_SLOT], idx_ref[3:4, 0:DY_SLOT]], axis=1)
    total = where_row.shape[1]
    pick_all[...] = jnp.where(iota((U_CAP, total), 0) == where_row, 1.0, 0.0).astype(BF16)
    sum_ref[...] = jnp.zeros_like(sum_ref)
    gain = gain_ref[...].astype(F32)
    ones = jnp.ones((U_CAP, 128), BF16)
    for c in copies:
        c.wait()

    def step(i, dg):
        at = pl.ds(pl.multiple_of(i * 128, 128), 128)
        pick = pick_all[:, at]
        h = dot(pick, u_ref[...], 0, 0)
        owned = dot(pick, ones, 0, 0)[:, 0:1] > 0.5
        r = lax.rsqrt(jnp.sum(h * h, axis=1, keepdims=True) * (1.0 / hidden) + RMS_EPS)
        xh = h * r
        dy = dy_all[at, :].astype(F32)
        u = dy * gain
        m = jnp.sum(u * xh, axis=1, keepdims=True) * (1.0 / hidden)
        dx = jnp.where(owned, r * (u - xh * m), 0.0).astype(BF16)
        sum_ref[...] += dot(pick, dx, 1, 0)
        return dg + jnp.sum((dy * xh).reshape(16, 8, hidden), axis=0)

    dg = lax.fori_loop(0, total // 128, step, jnp.zeros((8, hidden), F32))
    dg_ref[...] = jnp.sum(dg, axis=0, keepdims=True)


def slab_kernel(lst_ref, sum_ref, de_in, de_ref, stage, sem):
    del de_in
    count = lst_ref[2, 0]
    hidden = sum_ref.shape[1]
    sub = iota((SLAB, hidden), 0)

    def build(u, carry):
        lead = lst_ref[1, u]
        value = jnp.where(sub == (lst_ref[0, u] & 7), sum_ref[pl.ds(u, 1), :], 0.0)

        @pl.when(lead == u)
        def _():
            stage[u] = value

        @pl.when(lead != u)
        def _():
            stage[lead] += value

        return carry

    lax.fori_loop(0, count, build, 0)

    def send(u, carry):
        @pl.when(lst_ref[1, u] == u)
        def _():
            pltpu.make_async_copy(stage.at[u], de_ref.at[lst_ref[0, u] >> 3], sem).start()

        return carry

    lax.fori_loop(0, count, send, 0)

    def drain(u, carry):
        @pl.when(lst_ref[1, u] == u)
        def _():
            pltpu.make_async_copy(stage.at[u], de_ref.at[lst_ref[0, u] >> 3], sem).wait()

        return carry

    lax.fori_loop(0, count, drain, 0)


def zero_kernel(out_ref, zeros, sem):
    zeros[...] = jnp.zeros_like(zeros)
    step = zeros.shape[0]
    copies = [pltpu.make_async_copy(zeros, out_ref.at[pl.ds(i, step)], sem) for i in range(0, out_ref.shape[0], step)]
    for c in copies:
        c.start()
    for c in copies:
        c.wait()


def y_kernel(idx_ref, own_ref, sib_ref, got_ref, fwd_ref, gain_ref, g0, g1, g2, g3, y_ref, dg_ref, rows, sems):
    span, hidden = y_ref.shape
    copies = []
    at = 0
    for k, src in enumerate((own_ref, sib_ref, got_ref, fwd_ref)):
        copies.append(pltpu.make_async_copy(src, rows.at[pl.ds(at, src.shape[0])], sems.at[k]))
        copies[-1].start()
        at += src.shape[0]
    dg_ref[...] = (g0[...] + g1[...]) + (g2[...] + g3[...])
    pick = jnp.where(iota((rows.shape[0], span), 0) == idx_ref[1:2, 0:span], 1.0, 0.0).astype(BF16)
    for c in copies:
        c.wait()
    gain = gain_ref[...].astype(F32)
    for i in range(0, span, 128):
        h = dot(pick[:, i:i + 128], rows[...], 0, 0)
        r = lax.rsqrt(jnp.sum(h * h, axis=1, keepdims=True) * (1.0 / hidden) + RMS_EPS)
        y_ref[i:i + 128, :] = ((h * r).astype(BF16).astype(F32) * gain).astype(BF16)


def dense_step(token_ids, table_block, norm_gain, grad_block):
    rows_block, hidden = table_block.shape
    span = grad_block.shape[1]
    tp = lax.axis_index('tp')
    local_ids = token_ids[0] - tp * rows_block
    owned = (local_ids >= 0) & (local_ids < rows_block)
    looked_up = jnp.take(table_block, jnp.where(owned, local_ids, 0), axis=0)
    partial_rows = jnp.where(owned[:, None], looked_up, jnp.zeros((), BF16))
    embedded = lax.dynamic_slice(partial_rows, (tp * span, 0), (span, hidden))
    for flip in (1, 2, 3):
        block = lax.dynamic_slice(partial_rows, ((tp ^ flip) * span, 0), (span, hidden))
        embedded += lax.ppermute(block, 'tp', [(i, i ^ flip) for i in range(4)])
    h = embedded.astype(F32)
    r = lax.rsqrt(jnp.mean(h * h, axis=-1, keepdims=True) + RMS_EPS)
    xh = h * r
    y = xh.astype(BF16) * norm_gain
    dy = grad_block[0].astype(F32)
    dg = jnp.sum(dy * xh, axis=0)
    u = dy * norm_gain.astype(F32)
    dx = (r * (u - xh * jnp.mean(u * xh, axis=-1, keepdims=True))).astype(BF16)
    pair = dg + lax.ppermute(dg, 'tp', SIBLING)
    dg = pair + lax.ppermute(pair, 'tp', ACROSS)
    dx_all = jnp.zeros((4 * span, hidden), F32)
    for flip in (0, 1, 2, 3):
        block = dx if flip == 0 else lax.ppermute(dx, 'tp', [(i, i ^ flip) for i in range(4)])
        dx_all = lax.dynamic_update_slice(dx_all, block.astype(F32), ((tp ^ flip) * span, 0))
    segments = jnp.where(owned, local_ids, rows_block)
    de = jax.ops.segment_sum(dx_all, segments, num_segments=rows_block)
    return y, de, dg


def device_step(token_ids, table_block, norm_gain, grad_block):
    rows, hidden = table_block.shape
    n = token_ids.shape[1]
    span = grad_block.shape[1]
    dy = grad_block[0]
    gain = norm_gain.reshape(1, hidden)

    dy_sib = lax.ppermute(dy, 'tp', SIBLING)
    packed = pl.pallas_call(
        functools.partial(pack_kernel, rows), out_shape=jax.ShapeDtypeStruct((DY_CAP, hidden), BF16),
        in_specs=[VMEM, VMEM], out_specs=VMEM, cost_estimate=cost(2, 2 << 20), name='pack')(token_ids, dy)
    dy_got = lax.ppermute(packed, 'tp', ACROSS)
    idx, lst, over = pl.pallas_call(
        functools.partial(index_kernel, rows, span),
        out_shape=(jax.ShapeDtypeStruct((8, n), jnp.int32), jax.ShapeDtypeStruct((8, 256), jnp.int32),
                   jax.ShapeDtypeStruct((8, 128), F32)),
        in_specs=[VMEM], out_specs=(VMEM, VMEM, VMEM),
        scratch_shapes=[pltpu.VMEM((8, span), F32), pltpu.VMEM((8, n), F32)],
        cost_estimate=cost(3, 1 << 16), name='index')(token_ids)
    over = jnp.maximum(over, lax.ppermute(over, 'dp', [(i, i ^ 1) for i in range(4)]))
    over = jnp.maximum(over, lax.ppermute(over, 'dp', [(i, i ^ 2) for i in range(4)]))
    rows_u = pl.pallas_call(
        gather_kernel, out_shape=jax.ShapeDtypeStruct((U_CAP, hidden), BF16),
        in_specs=[SMEM, VMEM, ANY], out_specs=VMEM,
        scratch_shapes=[pltpu.VMEM((U_CAP, SLAB, hidden), BF16), pltpu.SemaphoreType.DMA],
        cost_estimate=cost(4, 6 << 20), name='gather')(lst, lst, table_block.reshape(rows // SLAB, SLAB, hidden))
    u_got = lax.ppermute(rows_u[:X_CAP], 'tp', ACROSS)
    u_sib = lax.ppermute(rows_u, 'tp', SIBLING)
    de = pl.pallas_call(
        zero_kernel, out_shape=jax.ShapeDtypeStruct((rows // SLAB, SLAB, hidden), F32),
        out_specs=ANY, scratch_shapes=[pltpu.VMEM((20, SLAB, hidden), F32), pltpu.SemaphoreType.DMA],
        cost_estimate=cost(20, 64 << 20), name='zero')()
    dy_fwd = lax.ppermute(dy_got, 'tp', SIBLING)
    sums, dg = pl.pallas_call(
        dx_kernel, out_shape=(jax.ShapeDtypeStruct((U_CAP, hidden), F32), jax.ShapeDtypeStruct((1, hidden), F32)),
        in_specs=[VMEM, ANY, ANY, ANY, ANY, VMEM, VMEM], out_specs=(VMEM, VMEM),
        scratch_shapes=[pltpu.VMEM((2 * span + 2 * DY_SLOT, hidden), BF16),
                        pltpu.VMEM((U_CAP, 2 * span + 2 * DY_SLOT), BF16), pltpu.SemaphoreType.DMA((4,))],
        cost_estimate=cost(7, 8 << 20), name='dx')(idx, dy, dy_sib, dy_got, dy_fwd, rows_u, gain)
    dgs = [dg] + [lax.ppermute(dg, 'tp', [(i, i ^ f) for i in range(4)]) for f in (1, 2, 3)]
    de = pl.pallas_call(
        slab_kernel, out_shape=jax.ShapeDtypeStruct((rows // SLAB, SLAB, hidden), F32),
        in_specs=[SMEM, VMEM, ANY], out_specs=ANY, input_output_aliases={2: 0},
        scratch_shapes=[pltpu.VMEM((U_CAP, SLAB, hidden), F32), pltpu.SemaphoreType.DMA],
        cost_estimate=cost(4, 8 << 20), name='slabs')(lst, sums, de)
    u_fwd = lax.ppermute(u_got, 'tp', SIBLING)
    y, dg = pl.pallas_call(
        y_kernel, out_shape=(jax.ShapeDtypeStruct((span, hidden), BF16), jax.ShapeDtypeStruct((1, hidden), F32)),
        in_specs=[VMEM, ANY, ANY, ANY, ANY, VMEM, VMEM, VMEM, VMEM, VMEM], out_specs=(VMEM, VMEM),
        scratch_shapes=[pltpu.VMEM((2 * U_CAP + 2 * X_CAP, hidden), BF16), pltpu.SemaphoreType.DMA((4,))],
        cost_estimate=cost(3, 4 << 20), name='y')(idx, rows_u, u_sib, u_got, u_fwd, gain, *dgs)

    def keep(y, de, dg):
        return y, de, dg

    def redo(y, de, dg):
        y, de, dg = dense_step(token_ids, table_block, norm_gain, grad_block)
        return y, de.reshape(rows // SLAB, SLAB, hidden), dg.reshape(1, hidden)

    y, de, dg = lax.cond(over[0, 0] > 0.5, redo, keep, y, de, dg)
    return y[None], de.reshape(rows, hidden), dg.reshape(hidden)


def solution(mesh):
    return jax.shard_map(device_step, mesh=mesh, in_specs=(P('dp', None), P('tp', None), P(None), P('dp', 'tp', None)), out_specs=(P('dp', 'tp', None), P(('dp', 'tp'), None), P('dp')), check_vma=False)
```

```python
import functools

import jax
import jax.numpy as jnp
from jax import lax
from jax.experimental import pallas as pl
from jax.experimental.pallas import tpu as pltpu
from jax.sharding import PartitionSpec as P


RMS_EPS = 1e-5
DY_CAP = 176
X_CAP = 96
U_CAP = 144
GROUP = 16
FILL_STEP = 20
BUILD = 4
FILLS = (0, 300, 500, 600, 860, 940, 1000)
SLAB = 8
KEY_STEP = 8192.0
NO_KEY = 1.0e6
ACROSS = [(i, i ^ 2) for i in range(4)]
SIBLING = [(i, i ^ 1) for i in range(4)]
F32 = jnp.float32
BF16 = jnp.bfloat16
ANY = pl.BlockSpec(memory_space=pltpu.HBM)
VMEM = pl.BlockSpec(memory_space=pltpu.VMEM)
SMEM = pl.BlockSpec(memory_space=pltpu.SMEM)


def dot(a, b, ca, cb):
    return lax.dot_general(a, b, (((ca,), (cb,)), ((), ())), preferred_element_type=F32)


def cost(us, moved):
    return pl.CostEstimate(flops=int(us * 2_000_000), bytes_accessed=moved, transcendentals=0)


def iota(shape, axis):
    return lax.broadcasted_iota(jnp.int32, shape, axis)


def owner_of(ids, rows):
    out = jnp.zeros_like(ids)
    for k in (1, 2, 3):
        out += jnp.where(ids >= k * rows, 1, 0)
    return out


def columns(row):
    parts = []
    for j in range(0, row.shape[1], 128):
        parts.append(jnp.broadcast_to(row[:, j:j + 128], (128, 128)).T)
    return jnp.concatenate(parts, axis=0)


def before(n):
    return jnp.where(iota((n, n), 0) < iota((n, n), 1), 1.0, 0.0).astype(BF16)


def pack_kernel(rows, ids_ref, dy_ref, out_ref):
    me = lax.axis_index('tp')
    span = dy_ref.shape[0]
    ids = ids_ref[:, pl.ds(pl.multiple_of(me * span, 128), span)]
    leaves = (owner_of(ids, rows) >= 2) != (me >= 2)
    flag = jnp.broadcast_to(jnp.where(leaves, 1.0, 0.0), (8, span))
    rank = dot(flag.astype(BF16), before(span), 1, 0)[0:1]
    rank = jnp.where(leaves, rank, -1.0)
    slots = iota((DY_CAP, span), 0).astype(F32)
    pick = jnp.where(slots == rank, 1.0, 0.0).astype(BF16)
    out_ref[...] = dot(pick, dy_ref[...], 1, 0).astype(BF16)


def index_tables(rows, span, ids, rank_ref, src_ref, idx_ref, lst_ref, flag_ref):
    me = lax.axis_index('tp')
    n = ids.shape[1]
    owner = owner_of(ids, rows)
    local = ids - owner * rows
    pos = iota((1, n), 1)
    idf = ids.astype(F32)
    col = columns(idf)
    posc = iota((n, 128), 0).astype(F32)
    lo, hi = [], []
    for j in range(0, n, 128):
        same = col == idf[:, j:j + 128]
        lo.append(jnp.min(jnp.where(same, posc, 4096.0), axis=0, keepdims=True))
        hi.append(jnp.max(jnp.where(same, posc, -1.0), axis=0, keepdims=True))
    lo = jnp.concatenate(lo, axis=1)
    hi = jnp.concatenate(hi, axis=1)
    first = lo == pos.astype(F32)
    half = n // 2
    wanted = jnp.where(owner < 2, jnp.where(hi >= half, 1.0, 0.0), jnp.where(lo < half, 1.0, 0.0))
    key = (owner.astype(F32) * 2.0 + 1.0 - wanted) * KEY_STEP + local.astype(F32)
    keyf = jnp.where(first, key, NO_KEY)
    kcol = columns(keyf)
    rank = []
    for j in range(0, n, 128):
        rank.append(jnp.sum(jnp.where(kcol < key[:, j:j + 128], 1.0, 0.0), axis=0, keepdims=True))
    rank = jnp.concatenate(rank, axis=1)

    def below(bound):
        return jnp.sum(jnp.where(keyf < bound, 1.0, 0.0), axis=1, keepdims=True)

    base = [below(2.0 * KEY_STEP * o) for o in range(5)]
    over = jnp.zeros((1, 1), F32)
    for o in range(4):
        over = jnp.maximum(over, jnp.where(base[o + 1] - base[o] > U_CAP, 1.0, 0.0))
        over = jnp.maximum(over, jnp.where(below((2.0 * o + 1.0) * KEY_STEP) - base[o] > X_CAP, 1.0, 0.0))
    start = jnp.where(owner == 0, base[0], jnp.where(owner == 1, base[1], jnp.where(owner == 2, base[2], base[3])))
    uidx = rank - start
    mine = owner == me
    uidx_mine = jnp.where(mine, uidx, -1.0)

    crosses = (owner >= 2) != (pos >= half)
    flag = jnp.where(crosses, 1.0, 0.0)
    flags = jnp.concatenate([flag[:, h * span:(h + 1) * span] for h in range(4)] + [jnp.zeros((4, span), F32)], axis=0)
    ranks = dot(flags.astype(BF16), before(span), 1, 0)
    over = jnp.maximum(over, jnp.max(jnp.where(jnp.sum(flags, axis=1, keepdims=True) > DY_CAP, 1.0, 0.0), axis=0, keepdims=True))
    rank_ref[...] = jnp.where(flags > 0.5, ranks, -1.0)
    src_ref[0:1, :] = uidx_mine
    rel = owner ^ me
    offset = jnp.where(rel == 0, 0, jnp.where(rel == 1, U_CAP, jnp.where(rel == 2, 2 * U_CAP, 2 * U_CAP + X_CAP)))
    src_ref[1:2, :] = uidx + offset.astype(F32)
    slots = iota((span, span), 0).astype(F32)
    for row, flip in ((2, 2), (3, 3)):
        h = me ^ flip
        there = pl.ds(pl.multiple_of(h * span, 128), span)
        pick = jnp.where(slots == rank_ref[pl.ds(h, 1), :], 1.0, 0.0).astype(BF16)
        value = jnp.broadcast_to(src_ref[0:1, there] + 1.0, (8, span)).astype(BF16)
        idx_ref[row:row + 1, :] = (dot(value, pick, 1, 1)[0:1] - 1.0).astype(jnp.int32)
    for row, flip in ((0, 0), (1, 1)):
        there = pl.ds(pl.multiple_of((me ^ flip) * span, 128), span)
        idx_ref[row:row + 1, :] = src_ref[0:1, there].astype(jnp.int32)
    idx_ref[4:5, :] = src_ref[1:2, pl.ds(pl.multiple_of(me * span, 128), span)].astype(jnp.int32)

    width = lst_ref.shape[1]
    lead_col = jnp.where(first & mine, uidx, -1.0)
    pick = jnp.where(iota((width, n), 0).astype(F32) == lead_col, 1.0, 0.0).astype(BF16)
    hi8 = local >> 8
    lo8 = local - hi8 * 256
    parts = jnp.concatenate([hi8.astype(F32), lo8.astype(F32), jnp.ones((1, n), F32), jnp.zeros((5, n), F32)], axis=0)
    got = dot(parts.astype(BF16), pick, 1, 1)
    row_of = got[0:1] * 256.0 + got[1:2]
    valid = got[2:3] > 0.5
    slab = jnp.where(valid, jnp.floor(row_of * (1.0 / SLAB)), -1.0)
    scol = columns(slab)
    slotc = iota((width, 128), 0).astype(F32)
    lead = []
    for j in range(0, width, 128):
        same = scol == slab[:, j:j + 128]
        lead.append(jnp.min(jnp.where(same, slotc, 4096.0), axis=0, keepdims=True))
    lead = jnp.where(valid, jnp.concatenate(lead, axis=1), -1.0)
    slot = iota((1, width), 1).astype(F32)
    heads = jnp.where(lead == slot, 1.0, 0.0)
    others = jnp.where(valid & (lead != slot), 1.0, 0.0)
    kinds = jnp.concatenate([heads, others, jnp.zeros((6, width), F32)], axis=0)
    place = dot(kinds.astype(BF16), before(width), 1, 0)
    slots = iota((width, width), 0).astype(F32)
    hi8 = jnp.floor(slab * (1.0 / 256.0))
    values = jnp.concatenate([slot, lead, hi8, slab - hi8 * 256.0, jnp.zeros((4, width), F32)], axis=0).astype(BF16)
    pick = jnp.where(slots == jnp.where(heads > 0.5, place[0:1], -1.0), 1.0, 0.0).astype(BF16)
    head = dot(values, pick, 1, 1)
    pick = jnp.where(slots == jnp.where(others > 0.5, place[1:2], -1.0), 1.0, 0.0).astype(BF16)
    other = dot(values, pick, 1, 1)
    counts = jnp.sum(jnp.concatenate([jnp.where(valid, 1.0, 0.0), kinds[0:7]], axis=0), axis=1, keepdims=True)
    counts = jnp.minimum(jnp.broadcast_to(counts, (8, width)), float(U_CAP))
    lanes = iota((1, width), 1)
    lst_ref[0:1, :] = row_of.astype(jnp.int32)
    lst_ref[1:2, :] = jnp.minimum(head[0:1], U_CAP - 1.0).astype(jnp.int32)
    lst_ref[2:3, :] = (head[2:3] * 256.0 + head[3:4]).astype(jnp.int32)
    lst_ref[3:4, :] = jnp.minimum(other[0:1], U_CAP - 1.0).astype(jnp.int32)
    lst_ref[4:5, :] = jnp.minimum(other[1:2], U_CAP - 1.0).astype(jnp.int32)
    lst_ref[5:6, :] = jnp.where(lanes == 0, counts[0:1], jnp.where(lanes == 1, counts[1:2], counts[2:3])).astype(jnp.int32)
    flag_ref[...] = jnp.broadcast_to(over, flag_ref.shape)


class Fill:
    def __init__(self, de_ref, zeros, sem):
        self.de_ref, self.zeros, self.sem, self.copies = de_ref, zeros, sem, []

    def clear(self):
        self.zeros[...] = jnp.zeros_like(self.zeros)

    def start(self, lo, hi):
        step = self.zeros.shape[0]
        for at in range(lo, hi, step):
            n = min(step, hi - at)
            self.copies.append(pltpu.make_async_copy(self.zeros.at[pl.ds(0, n)], self.de_ref.at[pl.ds(at, n)], self.sem))
            self.copies[-1].start()

    def wait(self):
        for c in self.copies:
            c.wait()


def inverse_rms(u_ref):
    h = u_ref[...].astype(F32)
    r = lax.rsqrt(jnp.sum(h * h, axis=1, keepdims=True) * (1.0 / h.shape[1]) + RMS_EPS)
    a = r.astype(BF16).astype(F32)
    b = (r - a).astype(BF16).astype(F32)
    parts = [jnp.broadcast_to(p, (h.shape[0], 128)) for p in (a, b, r - a - b)]
    return jnp.concatenate(parts, axis=1).astype(BF16)


def token_block(where_row, u_ref, cols, dy_ref, gain_ref, h_ref, r_ref, m_ref, dx_ref, dg_ref):
    n, hidden = dy_ref.shape
    pick = jnp.where(iota((U_CAP, n), 0) == where_row, 1.0, 0.0).astype(BF16)
    h_ref[0:n, :] = dot(pick, u_ref[...], 0, 0)
    r = dot(pick, cols, 0, 0)
    r_ref[0:n, :] = r[:, 0:128] + r[:, 128:256] + r[:, 256:384]

    def first(i, carry):
        at = pl.ds(pl.multiple_of(i * GROUP, GROUP), GROUP)
        r = r_ref[at, :]
        acc = jnp.zeros((GROUP, 128), F32)
        for j in range(0, hidden, 128):
            xh = h_ref[at, j:j + 128] * r
            dy = dy_ref[at, j:j + 128].astype(F32)
            acc += (dy * gain_ref[:, j:j + 128]) * xh
            dg_ref[:, j:j + 128] += jnp.sum((dy * xh).reshape(GROUP // 8, 8, 128), axis=0)
        m_ref[at, :] = acc
        return carry

    lax.fori_loop(0, n // GROUP, first, 0)
    m_ref[0:n, :] = jnp.broadcast_to(jnp.sum(m_ref[0:n, :], axis=1, keepdims=True) * (1.0 / hidden), (n, 128))

    def second(i, carry):
        at = pl.ds(pl.multiple_of(i * GROUP, GROUP), GROUP)
        r, m = r_ref[at, :], m_ref[at, :]
        for j in range(0, hidden, 128):
            xh = h_ref[at, j:j + 128] * r
            u = dy_ref[at, j:j + 128].astype(F32) * gain_ref[:, j:j + 128]
            dx_ref[at, j:j + 128] = jnp.where(r > 0.0, r * (u - xh * m), 0.0).astype(BF16)
        return carry

    lax.fori_loop(0, n // GROUP, second, 0)
    return dot(pick, dx_ref[0:n, :], 1, 0)


def main_kernel(rows, ids_ref, own_ref, table_ref, gain_ref, idx_ref, lst_ref, flag_ref, u_ref, ux_ref, sum_ref,
                dg_ref, de_ref, rank_ref, src_ref, lst_smem, slabs, h_ref, r_ref, m_ref, dx_ref, g_ref, zeros, sems):
    hidden = own_ref.shape[1]
    fill = Fill(de_ref, zeros, sems.at[0])
    fill.clear()
    fill.start(FILLS[0], FILLS[1])
    index_tables(rows, own_ref.shape[0], ids_ref[...], rank_ref, src_ref, idx_ref, lst_ref, flag_ref)
    c = pltpu.make_async_copy(lst_ref, lst_smem, sems.at[1])
    c.start()
    c.wait()

    def issue(u, carry):
        pltpu.make_async_copy(table_ref.at[lst_smem[0, u] >> 3], slabs.at[u], sems.at[2]).start()
        return carry

    lax.fori_loop(0, U_CAP, issue, 0, unroll=8)
    want = iota((1, U_CAP), 1) * SLAB + (lst_ref[0:1, 0:U_CAP] & 7)
    pick = jnp.where(iota((U_CAP * SLAB, U_CAP), 0) == want, 1.0, 0.0).astype(BF16)
    dg_ref[...] = jnp.zeros_like(dg_ref)
    g_ref[...] = gain_ref[...].reshape(1, hidden).astype(F32)
    pltpu.make_async_copy(table_ref.at[pl.ds(0, U_CAP)], slabs, sems.at[2]).wait()
    fill.start(FILLS[1], FILLS[2])
    u_ref[...] = dot(pick, slabs[...].reshape(U_CAP * SLAB, hidden), 0, 0).astype(BF16)
    ux_ref[...] = u_ref[0:X_CAP, :]
    cols = inverse_rms(u_ref)
    sum_ref[...] = token_block(idx_ref[0:1, :], u_ref, cols, own_ref, g_ref, h_ref, r_ref, m_ref, dx_ref, dg_ref)
    fill.wait()


def zero_kernel(lo, hi, de_in, de_ref, zeros, sem):
    del de_in
    fill = Fill(de_ref, zeros, sem)
    fill.clear()
    fill.start(lo, hi)
    fill.wait()


def token_kernel(idx_ref, u_ref, us_ref, sib_ref, got_ref, fwd_ref, sumin_ref, dgin_ref, gain_ref, de_in,
                 sum_ref, dg_ref, part_ref, de_ref, h_ref, r_ref, m_ref, dx_ref, dg8_ref, g_ref, zeros, sem):
    del de_in
    hidden = u_ref.shape[1]
    fill = Fill(de_ref, zeros, sem)
    fill.clear()
    fill.start(FILLS[3], FILLS[4])
    cols = inverse_rms(u_ref)
    g_ref[...] = gain_ref[...].reshape(1, hidden).astype(F32)
    dg8_ref[...] = dgin_ref[...]
    sum_ref[...] = sumin_ref[...] + token_block(idx_ref[1:2, :], u_ref, cols, sib_ref, g_ref, h_ref, r_ref, m_ref, dx_ref, dg8_ref)
    sum_ref[...] += token_block(idx_ref[2:3, 0:DY_CAP], u_ref, cols, got_ref, g_ref, h_ref, r_ref, m_ref, dx_ref, dg8_ref)
    sum_ref[...] += token_block(idx_ref[3:4, 0:DY_CAP], u_ref, cols, fwd_ref, g_ref, h_ref, r_ref, m_ref, dx_ref, dg8_ref)
    dg_ref[...] = jnp.sum(dg8_ref[...], axis=0, keepdims=True)
    src = idx_ref[4:5, :]
    span = src.shape[1]
    part = jnp.zeros((span, hidden), F32)
    for k, ref in enumerate((u_ref, us_ref)):
        pick = jnp.where(iota((U_CAP, span), 0) + k * U_CAP == src, 1.0, 0.0).astype(BF16)
        part += dot(pick, ref[...], 0, 0)
    part_ref[...] = part.astype(BF16)
    fill.wait()


def final_kernel(tab_ref, flag_ref, idx_ref, sum_ref, part_ref, got_ref, fwd_ref, gain_ref, g0, g1, g2, g3, de_in,
                 y_ref, dg_ref, over_ref, de_ref, lst_ref, stage, h_ref, r_ref, g_ref, zeros, sems):
    del de_in
    span, hidden = y_ref.shape
    table = pltpu.make_async_copy(tab_ref, lst_ref, sems.at[2])
    table.start()
    fill = Fill(de_ref, zeros, sems.at[0])
    fill.clear()
    fill.start(FILLS[5], FILLS[6])
    over_ref[...] = flag_ref[0:1, 0:1].astype(jnp.int32)
    dg_ref[...] = (g0[...] + g1[...]) + (g2[...] + g3[...])
    g_ref[...] = gain_ref[...].reshape(1, hidden).astype(F32)
    sub = iota((SLAB, hidden), 0)
    src = idx_ref[4:5, :] - 2 * U_CAP
    for k, ref in enumerate((got_ref, fwd_ref)):
        pick = jnp.where(iota((X_CAP, span), 0) + k * X_CAP == src, 1.0, 0.0).astype(BF16)
        h = dot(pick, ref[...], 0, 0)
        h_ref[...] = h if k == 0 else h_ref[...] + h
    table.wait()
    count, heads, others = lst_ref[5, 0], lst_ref[5, 1], lst_ref[5, 2]

    def build(i, carry):
        for k in range(BUILD):
            u = i * BUILD + k
            stage[u] = jnp.where(sub == (lst_ref[0, u] & 7), sum_ref[pl.ds(u, 1), :], 0.0)
        return carry

    lax.fori_loop(0, (count + BUILD - 1) // BUILD, build, 0)

    def join(i, carry):
        stage[lst_ref[4, i]] += stage[lst_ref[3, i]]
        return carry

    lax.fori_loop(0, others, join, 0)
    fill.wait()

    def send(i):
        pltpu.make_async_copy(stage.at[lst_ref[1, i]], de_ref.at[lst_ref[2, i]], sems.at[1]).start()

    def send_some(i, carry):
        for k in range(BUILD):
            send(i * BUILD + k)
        return carry

    def send_one(i, carry):
        send(i)
        return carry

    lax.fori_loop(0, heads // BUILD, send_some, 0)
    lax.fori_loop(heads // BUILD * BUILD, heads, send_one, 0)

    def first(i, carry):
        at = pl.ds(pl.multiple_of(i * GROUP, GROUP), GROUP)
        acc = jnp.zeros((GROUP, 128), F32)
        for j in range(0, hidden, 128):
            h = h_ref[at, j:j + 128] + part_ref[at, j:j + 128].astype(F32)
            h_ref[at, j:j + 128] = h
            acc += h * h
        r_ref[at, :] = acc
        return carry

    lax.fori_loop(0, span // GROUP, first, 0)
    r = lax.rsqrt(jnp.sum(r_ref[...], axis=1, keepdims=True) * (1.0 / hidden) + RMS_EPS)
    r_ref[...] = jnp.broadcast_to(r, (span, 128))

    def second(i, carry):
        at = pl.ds(pl.multiple_of(i * GROUP, GROUP), GROUP)
        r = r_ref[at, :]
        for j in range(0, hidden, 128):
            xh = (h_ref[at, j:j + 128] * r).astype(BF16).astype(F32)
            y_ref[at, j:j + 128] = (xh * g_ref[:, j:j + 128]).astype(BF16)
        return carry

    lax.fori_loop(0, span // GROUP, second, 0)
    pltpu.make_async_copy(stage.at[pl.ds(0, heads)], de_ref.at[pl.ds(0, heads)], sems.at[1]).wait()


def dense_step(token_ids, table_block, norm_gain, grad_block):
    rows_block, hidden = table_block.shape
    span = grad_block.shape[1]
    tp = lax.axis_index('tp')
    local_ids = token_ids[0] - tp * rows_block
    owned = (local_ids >= 0) & (local_ids < rows_block)
    looked_up = jnp.take(table_block, jnp.where(owned, local_ids, 0), axis=0)
    partial_rows = jnp.where(owned[:, None], looked_up, jnp.zeros((), BF16))
    embedded = lax.dynamic_slice(partial_rows, (tp * span, 0), (span, hidden))
    for flip in (1, 2, 3):
        block = lax.dynamic_slice(partial_rows, ((tp ^ flip) * span, 0), (span, hidden))
        embedded += lax.ppermute(block, 'tp', [(i, i ^ flip) for i in range(4)])
    h = embedded.astype(F32)
    r = lax.rsqrt(jnp.mean(h * h, axis=-1, keepdims=True) + RMS_EPS)
    xh = h * r
    y = xh.astype(BF16) * norm_gain
    dy = grad_block[0].astype(F32)
    dg = jnp.sum(dy * xh, axis=0)
    u = dy * norm_gain.astype(F32)
    dx = (r * (u - xh * jnp.mean(u * xh, axis=-1, keepdims=True))).astype(BF16)
    pair = dg + lax.ppermute(dg, 'tp', SIBLING)
    dg = pair + lax.ppermute(pair, 'tp', ACROSS)
    dx_all = jnp.zeros((4 * span, hidden), F32)
    for flip in (0, 1, 2, 3):
        block = dx if flip == 0 else lax.ppermute(dx, 'tp', [(i, i ^ flip) for i in range(4)])
        dx_all = lax.dynamic_update_slice(dx_all, block.astype(F32), ((tp ^ flip) * span, 0))
    segments = jnp.where(owned, local_ids, rows_block)
    de = jax.ops.segment_sum(dx_all, segments, num_segments=rows_block)
    return y, de, dg


def device_step(token_ids, table_block, norm_gain, grad_block):
    rows, hidden = table_block.shape
    span = grad_block.shape[1]
    dy = grad_block[0]
    slabs = rows // SLAB
    de_shape = jax.ShapeDtypeStruct((slabs, SLAB, hidden), F32)
    zeros = pltpu.VMEM((FILL_STEP, SLAB, hidden), F32)

    packed = pl.pallas_call(
        functools.partial(pack_kernel, rows), out_shape=jax.ShapeDtypeStruct((DY_CAP, hidden), BF16),
        in_specs=[VMEM, VMEM], out_specs=VMEM, compiler_params=pltpu.CompilerParams(vmem_limit_bytes=16 << 20),
        cost_estimate=cost(2, 2 << 20), name='pack')(token_ids, dy)
    dy_got = lax.ppermute(packed, 'tp', ACROSS)
    dy_held, packed = lax.optimization_barrier((dy, packed))
    dy_sib = lax.ppermute(dy_held, 'tp', SIBLING)
    idx, lst, over, rows_u, rows_x, sums, dg8, de = pl.pallas_call(
        functools.partial(main_kernel, rows),
        out_shape=(jax.ShapeDtypeStruct((8, span), jnp.int32), jax.ShapeDtypeStruct((8, 256), jnp.int32),
                   jax.ShapeDtypeStruct((8, 128), F32), jax.ShapeDtypeStruct((U_CAP, hidden), BF16),
                   jax.ShapeDtypeStruct((X_CAP, hidden), BF16), jax.ShapeDtypeStruct((U_CAP, hidden), F32),
                   jax.ShapeDtypeStruct((8, hidden), F32), de_shape),
        in_specs=[VMEM, VMEM, ANY, VMEM], out_specs=(VMEM,) * 7 + (ANY,),
        scratch_shapes=[pltpu.VMEM((8, span), F32), pltpu.VMEM((8, 4 * span), F32), pltpu.SMEM((8, 256), jnp.int32),
                        pltpu.VMEM((U_CAP, SLAB, hidden), BF16), pltpu.VMEM((span, hidden), F32),
                        pltpu.VMEM((span, 128), F32), pltpu.VMEM((span, 128), F32), pltpu.VMEM((span, hidden), BF16),
                        pltpu.VMEM((1, hidden), F32), zeros, pltpu.SemaphoreType.DMA((3,))],
        compiler_params=pltpu.CompilerParams(vmem_limit_bytes=36 << 20),
        cost_estimate=cost(12, 40 << 20), name='main')(
            token_ids, dy, table_block.reshape(slabs, SLAB, hidden), norm_gain)
    u_got = lax.ppermute(rows_x, 'tp', ACROSS)
    u_sib = lax.ppermute(rows_u, 'tp', SIBLING)

    def zero(de, lo, hi):
        return pl.pallas_call(
            functools.partial(zero_kernel, lo, hi), out_shape=de_shape, in_specs=[ANY], out_specs=ANY,
            input_output_aliases={0: 0}, scratch_shapes=[zeros, pltpu.SemaphoreType.DMA],
            compiler_params=pltpu.CompilerParams(vmem_limit_bytes=8 << 20),
            cost_estimate=cost(8, 20 << 20), name='zero')(de)

    de = zero(de, FILLS[2], FILLS[3])
    dy_got, over, de = lax.optimization_barrier((dy_got, over, de))
    dy_fwd = lax.ppermute(dy_got, 'tp', SIBLING)
    over = jnp.maximum(over, lax.ppermute(over, 'dp', [(i, i ^ 1) for i in range(4)]))
    sums, dg, part, de = pl.pallas_call(
        token_kernel,
        out_shape=(jax.ShapeDtypeStruct((U_CAP, hidden), F32), jax.ShapeDtypeStruct((1, hidden), F32),
                   jax.ShapeDtypeStruct((span, hidden), BF16), de_shape),
        in_specs=[VMEM] * 9 + [ANY], out_specs=(VMEM, VMEM, VMEM, ANY), input_output_aliases={9: 3},
        scratch_shapes=[pltpu.VMEM((span, hidden), F32), pltpu.VMEM((span, 128), F32), pltpu.VMEM((span, 128), F32),
                        pltpu.VMEM((span, hidden), BF16), pltpu.VMEM((8, hidden), F32), pltpu.VMEM((1, hidden), F32),
                        zeros, pltpu.SemaphoreType.DMA],
        compiler_params=pltpu.CompilerParams(vmem_limit_bytes=32 << 20),
        cost_estimate=cost(8, 16 << 20), name='tokens')(
            idx, rows_u, u_sib, dy_sib, dy_got, dy_fwd, sums, dg8, norm_gain, de)
    dgs = [dg]
    for f in (1, 2, 3):
        dgs.append(lax.ppermute(dg, 'tp', [(i, i ^ f) for i in range(4)]))
    u_got, part, over = lax.optimization_barrier((u_got, part, over))
    u_fwd = lax.ppermute(u_got, 'tp', SIBLING)
    over = jnp.maximum(over, lax.ppermute(over, 'dp', [(i, i ^ 2) for i in range(4)]))
    if FILLS[5] > FILLS[4]:
        de = zero(de, FILLS[4], FILLS[5])
    y, dg, over, de = pl.pallas_call(
        final_kernel,
        out_shape=(jax.ShapeDtypeStruct((span, hidden), BF16), jax.ShapeDtypeStruct((1, hidden), F32),
                   jax.ShapeDtypeStruct((1, 1), jnp.int32), de_shape),
        in_specs=[VMEM] * 12 + [ANY], out_specs=(VMEM, VMEM, VMEM, ANY), input_output_aliases={12: 3},
        scratch_shapes=[pltpu.SMEM((8, 256), jnp.int32), pltpu.VMEM((U_CAP, SLAB, hidden), F32), pltpu.VMEM((span, hidden), F32),
                        pltpu.VMEM((span, 128), F32), pltpu.VMEM((1, hidden), F32), zeros, pltpu.SemaphoreType.DMA((3,))],
        compiler_params=pltpu.CompilerParams(vmem_limit_bytes=32 << 20),
        cost_estimate=cost(5, 8 << 20), name='final')(lst, over, idx, sums, part, u_got, u_fwd, norm_gain, *dgs, de)

    def keep(y, de, dg):
        return y, de, dg

    def redo(y, de, dg):
        y, de, dg = dense_step(token_ids, table_block, norm_gain, grad_block)
        return y, de.reshape(slabs, SLAB, hidden), dg.reshape(1, hidden)

    y, de, dg = lax.cond(over.reshape(()) > 0, redo, keep, y, de, dg)
    return y[None], de.reshape(rows, hidden), dg.reshape(hidden)


def solution(mesh):
    return jax.shard_map(device_step, mesh=mesh, in_specs=(P('dp', None), P('tp', None), P(None), P('dp', 'tp', None)), out_specs=(P('dp', 'tp', None), P(('dp', 'tp'), None), P('dp')), check_vma=False)
```

```python
import functools

import jax
import jax.numpy as jnp
from jax import lax
from jax.experimental import pallas as pl
from jax.experimental.pallas import tpu as pltpu
from jax.sharding import PartitionSpec as P


RMS_EPS = 1e-5
DY_CAP = 176
X_CAP = 96
U_CAP = 144
GROUP = 16
FILL_STEP = 10
BUILD = 4
FILLS = (0, 380, 560, 570, 640, 900, 960, 1000)
SLAB = 8
KEY_STEP = 8192.0
NO_KEY = 1.0e6
ACROSS = [(i, i ^ 2) for i in range(4)]
SIBLING = [(i, i ^ 1) for i in range(4)]
F32 = jnp.float32
BF16 = jnp.bfloat16
ANY = pl.BlockSpec(memory_space=pltpu.HBM)
VMEM = pl.BlockSpec(memory_space=pltpu.VMEM)
SMEM = pl.BlockSpec(memory_space=pltpu.SMEM)


def dot(a, b, ca, cb):
    return lax.dot_general(a, b, (((ca,), (cb,)), ((), ())), preferred_element_type=F32)


def mm(a, b):
    return dot(a, b, 1, 0)


def mt(a, b):
    return dot(a, b, 1, 1)


def tm(a, b):
    return dot(a, b, 0, 0)


def num(test):
    return jnp.where(test, 1.0, 0.0)


def line(k):
    return slice(k, k + 1)


def down(f, x):
    return f(x, axis=0, keepdims=True)


def along(f, x):
    return f(x, axis=1, keepdims=True)


def cost(us, moved):
    return pl.CostEstimate(flops=int(us * 2_000_000), bytes_accessed=moved, transcendentals=0)


def iota(shape, axis):
    return lax.broadcasted_iota(jnp.int32, shape, axis)


def owner_of(ids, rows):
    out = jnp.zeros_like(ids)
    for k in (1, 2, 3):
        out += jnp.where(ids >= k * rows, 1, 0)
    return out


def columns(row):
    parts = []
    for j in range(0, row.shape[1], 128):
        parts.append(jnp.broadcast_to(row[:, j:j + 128], (128, 128)).T)
    return jnp.concatenate(parts, axis=0)


def before(n):
    return num(iota((n, n), 0) < iota((n, n), 1)).astype(BF16)


def pack_kernel(rows, ids_ref, dy_ref, out_ref):
    me = lax.axis_index('tp')
    span = dy_ref.shape[0]
    ids = ids_ref[:, pl.ds(pl.multiple_of(me * span, 128), span)]
    leaves = (owner_of(ids, rows) >= 2) != (me >= 2)
    flag = jnp.broadcast_to(num(leaves), (8, span))
    rank = mm(flag.astype(BF16), before(span))[line(0)]
    rank = jnp.where(leaves, rank, -1.0)
    slots = iota((DY_CAP, span), 0).astype(F32)
    pick = num(slots == rank).astype(BF16)
    out_ref[...] = mm(pick, dy_ref[...]).astype(BF16)


def owned_rows(rows, ids, lst_ref):
    me = lax.axis_index('tp')
    n = ids.shape[1]
    owner = owner_of(ids, rows)
    local = ids - owner * rows
    pos = iota((1, n), 1)
    idf = ids.astype(F32)
    col = columns(idf)
    posc = iota((n, 128), 0).astype(F32)
    lo, hi = [], []
    for j in range(0, n, 128):
        same = col == idf[:, j:j + 128]
        lo.append(down(jnp.min, jnp.where(same, posc, 4096.0)))
        hi.append(down(jnp.max, jnp.where(same, posc, -1.0)))
    lo = jnp.concatenate(lo, axis=1)
    hi = jnp.concatenate(hi, axis=1)
    first = lo == pos.astype(F32)
    half = n // 2
    wanted = jnp.where(owner < 2, num(hi >= half), num(lo < half))
    key = (owner.astype(F32) * 2.0 + 1.0 - wanted) * KEY_STEP + local.astype(F32)
    keyf = jnp.where(first, key, NO_KEY)
    kcol = columns(keyf)
    rank = []
    for j in range(0, n, 128):
        rank.append(down(jnp.sum, jnp.where(kcol < key[:, j:j + 128], 1.0, 0.0)))
    rank = jnp.concatenate(rank, axis=1)

    def below(bound):
        return along(jnp.sum, num(keyf < bound))

    base = [below(2.0 * KEY_STEP * o) for o in range(5)]
    over = jnp.zeros((1, 1), F32)
    for o in range(4):
        over = jnp.maximum(over, num(base[o + 1] - base[o] > U_CAP))
        over = jnp.maximum(over, num(below((2.0 * o + 1.0) * KEY_STEP) - base[o] > X_CAP))
    start = jnp.where(owner == 0, base[0], jnp.where(owner == 1, base[1], jnp.where(owner == 2, base[2], base[3])))
    uidx = rank - start
    mine = owner == me
    uidx_mine = jnp.where(mine, uidx, -1.0)

    width = lst_ref.shape[1]
    lead_col = jnp.where(first & mine, uidx, -1.0)
    pick = num(iota((width, n), 0).astype(F32) == lead_col).astype(BF16)
    hi8 = local >> 8
    lo8 = local - hi8 * 256
    parts = jnp.concatenate([hi8.astype(F32), lo8.astype(F32), jnp.ones((1, n), F32), jnp.zeros((5, n), F32)], axis=0)
    got = mt(parts.astype(BF16), pick)
    row_of = got[line(0)] * 256.0 + got[line(1)]
    valid = got[line(2)] > 0.5
    spare = iota(row_of.shape, 1) * SLAB
    lst_ref[line(0), :] = jnp.where(valid, row_of.astype(jnp.int32), spare)
    return me, owner, pos, uidx, uidx_mine, over, row_of, valid


def other_tables(span, found, rank_ref, src_ref, idx_ref, lst_ref, flag_ref):
    me, owner, pos, uidx, uidx_mine, over, row_of, valid = found
    n = pos.shape[1]
    half = n // 2
    width = lst_ref.shape[1]
    crosses = (owner >= 2) != (pos >= half)
    flag = num(crosses)
    flags = jnp.concatenate([flag[:, h * span:(h + 1) * span] for h in range(4)] + [jnp.zeros((4, span), F32)], axis=0)
    ranks = mm(flags.astype(BF16), before(span))
    over = jnp.maximum(over, down(jnp.max, num(along(jnp.sum, flags) > DY_CAP)))
    rank_ref[...] = jnp.where(flags > 0.5, ranks, -1.0)
    src_ref[line(0), :] = uidx_mine
    rel = owner ^ me
    offset = jnp.where(rel == 0, 0, jnp.where(rel == 1, U_CAP, jnp.where(rel == 2, 2 * U_CAP, 2 * U_CAP + X_CAP)))
    src_ref[line(1), :] = uidx + offset.astype(F32)
    slots = iota((span, span), 0).astype(F32)
    for row, flip in ((2, 2), (3, 3)):
        h = me ^ flip
        there = pl.ds(pl.multiple_of(h * span, 128), span)
        pick = jnp.where(slots == rank_ref[pl.ds(h, 1), :], 1.0, 0.0).astype(BF16)
        value = jnp.broadcast_to(src_ref[line(0), there] + 1.0, (8, span)).astype(BF16)
        idx_ref[line(row), :] = (mt(value, pick)[line(0)] - 1.0).astype(jnp.int32)
    for row, flip in ((0, 0), (1, 1)):
        there = pl.ds(pl.multiple_of((me ^ flip) * span, 128), span)
        idx_ref[line(row), :] = src_ref[line(0), there].astype(jnp.int32)
    idx_ref[line(4), :] = src_ref[line(1), pl.ds(pl.multiple_of(me * span, 128), span)].astype(jnp.int32)

    slab = jnp.where(valid, jnp.floor(row_of * (1.0 / SLAB)), -1.0)
    scol = columns(slab)
    slotc = iota((width, 128), 0).astype(F32)
    lead = []
    for j in range(0, width, 128):
        same = scol == slab[:, j:j + 128]
        lead.append(down(jnp.min, jnp.where(same, slotc, 4096.0)))
    lead = jnp.where(valid, jnp.concatenate(lead, axis=1), -1.0)
    slot = iota((1, width), 1).astype(F32)
    heads = num(lead == slot)
    others = num(valid & (lead != slot))
    kinds = jnp.concatenate([heads, others, jnp.zeros((6, width), F32)], axis=0)
    place = mm(kinds.astype(BF16), before(width))
    slots = iota((width, width), 0).astype(F32)
    hi8 = jnp.floor(slab * (1.0 / 256.0))
    values = jnp.concatenate([slot, lead, hi8, slab - hi8 * 256.0, jnp.zeros((4, width), F32)], axis=0).astype(BF16)
    pick = num(slots == jnp.where(heads > 0.5, place[line(0)], -1.0)).astype(BF16)
    head = mt(values, pick)
    pick = num(slots == jnp.where(others > 0.5, place[line(1)], -1.0)).astype(BF16)
    other = mt(values, pick)
    counts = along(jnp.sum, jnp.concatenate([num(valid), kinds[0:7]], axis=0))
    counts = jnp.minimum(jnp.broadcast_to(counts, (8, width)), float(U_CAP))
    lanes = iota((1, width), 1)
    lst_ref[line(1), :] = jnp.minimum(head[line(0)], U_CAP - 1.0).astype(jnp.int32)
    lst_ref[line(2), :] = (head[line(2)] * 256.0 + head[line(3)]).astype(jnp.int32)
    lst_ref[line(3), :] = jnp.minimum(other[line(0)], U_CAP - 1.0).astype(jnp.int32)
    lst_ref[line(4), :] = jnp.minimum(other[line(1)], U_CAP - 1.0).astype(jnp.int32)
    lst_ref[line(5), :] = jnp.where(lanes == 0, counts[line(0)], jnp.where(lanes == 1, counts[line(1)], counts[line(2)])).astype(jnp.int32)
    flag_ref[...] = jnp.broadcast_to(over, flag_ref.shape)


class Fill:
    def __init__(self, de_ref, zeros, sem):
        self.de_ref, self.zeros, self.sem, self.copies = de_ref, zeros, sem, []

    def clear(self):
        self.zeros[...] = jnp.zeros_like(self.zeros)

    def start(self, lo, hi):
        step = self.zeros.shape[0]
        for at in range(lo, hi, step):
            n = min(step, hi - at)
            self.copies.append(pltpu.make_async_copy(self.zeros.at[pl.ds(0, n)], self.de_ref.at[pl.ds(at, n)], self.sem))
            self.copies[-1].start()

    def wait(self):
        for c in self.copies:
            c.wait()


def inverse_rms(u_ref):
    h = u_ref[...].astype(F32)
    r = lax.rsqrt(along(jnp.sum, h * h) * (1.0 / h.shape[1]) + RMS_EPS)
    a = r.astype(BF16).astype(F32)
    b = (r - a).astype(BF16).astype(F32)
    parts = [jnp.broadcast_to(p, (h.shape[0], 128)) for p in (a, b, r - a - b)]
    return jnp.concatenate(parts, axis=1).astype(BF16)


def token_block(where_row, u_ref, cols, dy_ref, gain_ref, h_ref, r_ref, m_ref, dx_ref, dg_ref):
    n, hidden = dy_ref.shape
    pick = num(iota((U_CAP, n), 0) == where_row).astype(BF16)
    h_ref[0:n, :] = tm(pick, u_ref[...])
    r = tm(pick, cols)
    r_ref[0:n, :] = r[:, 0:128] + r[:, 128:256] + r[:, 256:384]

    def first(i, carry):
        at = pl.ds(pl.multiple_of(i * GROUP, GROUP), GROUP)
        r = r_ref[at, :]
        acc = jnp.zeros((GROUP, 128), F32)
        for j in range(0, hidden, 128):
            xh = h_ref[at, j:j + 128] * r
            dy = dy_ref[at, j:j + 128].astype(F32)
            acc += (dy * gain_ref[:, j:j + 128]) * xh
            dg_ref[:, j:j + 128] += jnp.sum((dy * xh).reshape(GROUP // 8, 8, 128), axis=0)
        m_ref[at, :] = acc
        return carry

    lax.fori_loop(0, n // GROUP, first, 0)
    m_ref[0:n, :] = jnp.broadcast_to(along(jnp.sum, m_ref[0:n, :]) * (1.0 / hidden), (n, 128))

    def second(i, carry):
        at = pl.ds(pl.multiple_of(i * GROUP, GROUP), GROUP)
        r, m = r_ref[at, :], m_ref[at, :]
        for j in range(0, hidden, 128):
            xh = h_ref[at, j:j + 128] * r
            u = dy_ref[at, j:j + 128].astype(F32) * gain_ref[:, j:j + 128]
            dx_ref[at, j:j + 128] = jnp.where(r > 0.0, r * (u - xh * m), 0.0).astype(BF16)
        return carry

    lax.fori_loop(0, n // GROUP, second, 0)
    return mm(pick, dx_ref[0:n, :])


def main_kernel(rows, ids_ref, own_ref, table_ref, gain_ref, idx_ref, lst_ref, flag_ref, u_ref, ux_ref, sum_ref,
                dg_ref, de_ref, rank_ref, src_ref, row_ref, lst_smem, slabs, h_ref, r_ref, m_ref, dx_ref, g_ref, zeros, sems):
    hidden = own_ref.shape[1]
    fill = Fill(de_ref, zeros, sems.at[0])
    fill.clear()
    fill.start(FILLS[0], FILLS[1])
    found = owned_rows(rows, ids_ref[...], row_ref)
    c = pltpu.make_async_copy(row_ref, lst_smem, sems.at[1])
    c.start()
    c.wait()

    def issue(u, carry):
        pltpu.make_async_copy(table_ref.at[lst_smem[0, u] >> 3], slabs.at[u], sems.at[2]).start()
        return carry

    lax.fori_loop(0, U_CAP, issue, 0, unroll=8)
    want = iota((1, U_CAP), 1) * SLAB + (row_ref[line(0), 0:U_CAP] & 7)
    pick = num(iota((U_CAP * SLAB, U_CAP), 0) == want).astype(BF16)
    dg_ref[...] = jnp.zeros_like(dg_ref)
    g_ref[...] = gain_ref[...].reshape(1, hidden).astype(F32)
    lst_ref[...] = row_ref[...]
    other_tables(own_ref.shape[0], found, rank_ref, src_ref, idx_ref, lst_ref, flag_ref)
    pltpu.make_async_copy(table_ref.at[pl.ds(0, U_CAP)], slabs, sems.at[2]).wait()
    fill.start(FILLS[1], FILLS[2])
    u_ref[...] = tm(pick, slabs[...].reshape(U_CAP * SLAB, hidden)).astype(BF16)
    ux_ref[...] = u_ref[0:X_CAP, :]
    cols = inverse_rms(u_ref)
    sum_ref[...] = token_block(idx_ref[line(0), :], u_ref, cols, own_ref, g_ref, h_ref, r_ref, m_ref, dx_ref, dg_ref)
    fill.wait()


def zero_kernel(lo, hi, de_in, de_ref, zeros, sem):
    del de_in
    fill = Fill(de_ref, zeros, sem)
    fill.clear()
    fill.start(lo, hi)
    fill.wait()


def token_kernel(idx_ref, u_ref, us_ref, sib_ref, got_ref, fwd_ref, sumin_ref, dgin_ref, gain_ref, de_in,
                 sum_ref, dg_ref, part_ref, de_ref, h_ref, r_ref, m_ref, dx_ref, dg8_ref, g_ref, zeros, sem):
    del de_in
    hidden = u_ref.shape[1]
    fill = Fill(de_ref, zeros, sem)
    fill.clear()
    fill.start(FILLS[4], FILLS[5])
    cols = inverse_rms(u_ref)
    g_ref[...] = gain_ref[...].reshape(1, hidden).astype(F32)
    dg8_ref[...] = dgin_ref[...]
    sum_ref[...] = sumin_ref[...] + token_block(idx_ref[line(1), :], u_ref, cols, sib_ref, g_ref, h_ref, r_ref, m_ref, dx_ref, dg8_ref)
    sum_ref[...] += token_block(idx_ref[line(2), 0:DY_CAP], u_ref, cols, got_ref, g_ref, h_ref, r_ref, m_ref, dx_ref, dg8_ref)
    sum_ref[...] += token_block(idx_ref[line(3), 0:DY_CAP], u_ref, cols, fwd_ref, g_ref, h_ref, r_ref, m_ref, dx_ref, dg8_ref)
    dg_ref[...] = down(jnp.sum, dg8_ref[...])
    src = idx_ref[line(4), :]
    span = src.shape[1]
    part = jnp.zeros((span, hidden), F32)
    for k, ref in enumerate((u_ref, us_ref)):
        pick = num(iota((U_CAP, span), 0) + k * U_CAP == src).astype(BF16)
        part += tm(pick, ref[...])
    part_ref[...] = part.astype(BF16)
    fill.wait()


def final_kernel(tab_ref, flag_ref, idx_ref, sum_ref, part_ref, got_ref, fwd_ref, gain_ref, g0, g1, g2, g3, de_in,
                 y_ref, dg_ref, over_ref, de_ref, lst_ref, stage, h_ref, r_ref, g_ref, zeros, sems):
    del de_in
    span, hidden = y_ref.shape
    table = pltpu.make_async_copy(tab_ref, lst_ref, sems.at[2])
    table.start()
    fill = Fill(de_ref, zeros, sems.at[0])
    fill.clear()
    fill.start(FILLS[6], FILLS[7])
    over_ref[...] = flag_ref[line(0), 0:1].astype(jnp.int32)
    dg_ref[...] = (g0[...] + g1[...]) + (g2[...] + g3[...])
    g_ref[...] = gain_ref[...].reshape(1, hidden).astype(F32)
    sub = iota((SLAB, hidden), 0)
    table.wait()
    count, heads, others = lst_ref[5, 0], lst_ref[5, 1], lst_ref[5, 2]

    def build(i, carry):
        for k in range(BUILD):
            u = i * BUILD + k
            stage[u] = jnp.where(sub == (lst_ref[0, u] & 7), sum_ref[pl.ds(u, 1), :], 0.0)
        return carry

    lax.fori_loop(0, (count + BUILD - 1) // BUILD, build, 0)

    def join(i, carry):
        stage[lst_ref[4, i]] += stage[lst_ref[3, i]]
        return carry

    lax.fori_loop(0, others, join, 0)
    fill.wait()

    def send(i):
        pltpu.make_async_copy(stage.at[lst_ref[1, i]], de_ref.at[lst_ref[2, i]], sems.at[1]).start()

    def send_some(i, carry):
        for k in range(BUILD):
            send(i * BUILD + k)
        return carry

    def send_one(i, carry):
        send(i)
        return carry

    lax.fori_loop(0, heads // BUILD, send_some, 0)
    lax.fori_loop(heads // BUILD * BUILD, heads, send_one, 0)
    src = idx_ref[line(4), :] - 2 * U_CAP
    for k, ref in enumerate((got_ref, fwd_ref)):
        pick = num(iota((X_CAP, span), 0) + k * X_CAP == src).astype(BF16)
        h = tm(pick, ref[...])
        h_ref[...] = h if k == 0 else h_ref[...] + h

    def first(i, carry):
        at = pl.ds(pl.multiple_of(i * GROUP, GROUP), GROUP)
        acc = jnp.zeros((GROUP, 128), F32)
        for j in range(0, hidden, 128):
            h = h_ref[at, j:j + 128] + part_ref[at, j:j + 128].astype(F32)
            h_ref[at, j:j + 128] = h
            acc += h * h
        r_ref[at, :] = acc
        return carry

    lax.fori_loop(0, span // GROUP, first, 0)
    r = lax.rsqrt(along(jnp.sum, r_ref[...]) * (1.0 / hidden) + RMS_EPS)
    r_ref[...] = jnp.broadcast_to(r, (span, 128))

    def second(i, carry):
        at = pl.ds(pl.multiple_of(i * GROUP, GROUP), GROUP)
        r = r_ref[at, :]
        for j in range(0, hidden, 128):
            xh = (h_ref[at, j:j + 128] * r).astype(BF16).astype(F32)
            y_ref[at, j:j + 128] = (xh * g_ref[:, j:j + 128]).astype(BF16)
        return carry

    lax.fori_loop(0, span // GROUP, second, 0)
    pltpu.make_async_copy(stage.at[pl.ds(0, heads)], de_ref.at[pl.ds(0, heads)], sems.at[1]).wait()


def dense_step(token_ids, table_block, norm_gain, grad_block):
    rows_block, hidden = table_block.shape
    span = grad_block.shape[1]
    tp = lax.axis_index('tp')
    local_ids = token_ids[0] - tp * rows_block
    owned = (local_ids >= 0) & (local_ids < rows_block)
    looked_up = jnp.take(table_block, jnp.where(owned, local_ids, 0), axis=0)
    partial_rows = jnp.where(owned[:, None], looked_up, jnp.zeros((), BF16))
    embedded = lax.dynamic_slice(partial_rows, (tp * span, 0), (span, hidden))
    for flip in (1, 2, 3):
        block = lax.dynamic_slice(partial_rows, ((tp ^ flip) * span, 0), (span, hidden))
        embedded += lax.ppermute(block, 'tp', [(i, i ^ flip) for i in range(4)])
    h = embedded.astype(F32)
    r = lax.rsqrt(jnp.mean(h * h, axis=-1, keepdims=True) + RMS_EPS)
    xh = h * r
    y = xh.astype(BF16) * norm_gain
    dy = grad_block[0].astype(F32)
    dg = jnp.sum(dy * xh, axis=0)
    u = dy * norm_gain.astype(F32)
    dx = (r * (u - xh * jnp.mean(u * xh, axis=-1, keepdims=True))).astype(BF16)
    pair = dg + lax.ppermute(dg, 'tp', SIBLING)
    dg = pair + lax.ppermute(pair, 'tp', ACROSS)
    dx_all = jnp.zeros((4 * span, hidden), F32)
    for flip in (0, 1, 2, 3):
        block = dx if flip == 0 else lax.ppermute(dx, 'tp', [(i, i ^ flip) for i in range(4)])
        dx_all = lax.dynamic_update_slice(dx_all, block.astype(F32), ((tp ^ flip) * span, 0))
    segments = jnp.where(owned, local_ids, rows_block)
    de = jax.ops.segment_sum(dx_all, segments, num_segments=rows_block)
    return y, de, dg


def device_step(token_ids, table_block, norm_gain, grad_block):
    rows, hidden = table_block.shape
    span = grad_block.shape[1]
    dy = grad_block[0]
    slabs = rows // SLAB
    de_shape = jax.ShapeDtypeStruct((slabs, SLAB, hidden), F32)
    zeros = pltpu.VMEM((FILL_STEP, SLAB, hidden), F32)

    packed = pl.pallas_call(
        functools.partial(pack_kernel, rows), out_shape=jax.ShapeDtypeStruct((DY_CAP, hidden), BF16),
        in_specs=[VMEM, VMEM], out_specs=VMEM, compiler_params=pltpu.CompilerParams(vmem_limit_bytes=16 << 20),
        cost_estimate=cost(2, 2 << 20), name='pack')(token_ids, dy)
    dy_got = lax.ppermute(packed, 'tp', ACROSS)
    dy_held, packed = lax.optimization_barrier((dy, packed))
    dy_sib = lax.ppermute(dy_held, 'tp', SIBLING)
    idx, lst, over, rows_u, rows_x, sums, dg8, de = pl.pallas_call(
        functools.partial(main_kernel, rows),
        out_shape=(jax.ShapeDtypeStruct((8, span), jnp.int32), jax.ShapeDtypeStruct((8, 256), jnp.int32),
                   jax.ShapeDtypeStruct((8, 128), F32), jax.ShapeDtypeStruct((U_CAP, hidden), BF16),
                   jax.ShapeDtypeStruct((X_CAP, hidden), BF16), jax.ShapeDtypeStruct((U_CAP, hidden), F32),
                   jax.ShapeDtypeStruct((8, hidden), F32), de_shape),
        in_specs=[VMEM, VMEM, ANY, VMEM], out_specs=(VMEM,) * 7 + (ANY,),
        scratch_shapes=[pltpu.VMEM((8, span), F32), pltpu.VMEM((8, 4 * span), F32), pltpu.VMEM((8, 256), jnp.int32),
                        pltpu.SMEM((8, 256), jnp.int32),
                        pltpu.VMEM((U_CAP, SLAB, hidden), BF16), pltpu.VMEM((span, hidden), F32),
                        pltpu.VMEM((span, 128), F32), pltpu.VMEM((span, 128), F32), pltpu.VMEM((span, hidden), BF16),
                        pltpu.VMEM((1, hidden), F32), zeros, pltpu.SemaphoreType.DMA((3,))],
        compiler_params=pltpu.CompilerParams(vmem_limit_bytes=36 << 20),
        cost_estimate=cost(12, 40 << 20), name='main')(
            token_ids, dy, table_block.reshape(slabs, SLAB, hidden), norm_gain)
    u_got = lax.ppermute(rows_x, 'tp', ACROSS)
    u_sib = lax.ppermute(rows_u, 'tp', SIBLING)

    def zero(de, lo, hi):
        return pl.pallas_call(
            functools.partial(zero_kernel, lo, hi), out_shape=de_shape, in_specs=[ANY], out_specs=ANY,
            input_output_aliases={0: 0}, scratch_shapes=[zeros, pltpu.SemaphoreType.DMA],
            compiler_params=pltpu.CompilerParams(vmem_limit_bytes=8 << 20),
            cost_estimate=cost(8, 20 << 20), name='zero')(de)

    de = zero(de, FILLS[2], FILLS[3])
    dy_got, over, de = lax.optimization_barrier((dy_got, over, de))
    dy_fwd = lax.ppermute(dy_got, 'tp', SIBLING)
    over = jnp.maximum(over, lax.ppermute(over, 'dp', [(i, i ^ 1) for i in range(4)]))
    de = zero(de, FILLS[3], FILLS[4])
    sums, dg, part, de = pl.pallas_call(
        token_kernel,
        out_shape=(jax.ShapeDtypeStruct((U_CAP, hidden), F32), jax.ShapeDtypeStruct((1, hidden), F32),
                   jax.ShapeDtypeStruct((span, hidden), BF16), de_shape),
        in_specs=[VMEM] * 9 + [ANY], out_specs=(VMEM, VMEM, VMEM, ANY), input_output_aliases={9: 3},
        scratch_shapes=[pltpu.VMEM((span, hidden), F32), pltpu.VMEM((span, 128), F32), pltpu.VMEM((span, 128), F32),
                        pltpu.VMEM((span, hidden), BF16), pltpu.VMEM((8, hidden), F32), pltpu.VMEM((1, hidden), F32),
                        zeros, pltpu.SemaphoreType.DMA],
        compiler_params=pltpu.CompilerParams(vmem_limit_bytes=32 << 20),
        cost_estimate=cost(8, 16 << 20), name='tokens')(
            idx, rows_u, u_sib, dy_sib, dy_got, dy_fwd, sums, dg8, norm_gain, de)
    dgs = [dg]
    for f in (1, 2, 3):
        dgs.append(lax.ppermute(dg, 'tp', [(i, i ^ f) for i in range(4)]))
    u_got, part, over = lax.optimization_barrier((u_got, part, over))
    u_fwd = lax.ppermute(u_got, 'tp', SIBLING)
    over = jnp.maximum(over, lax.ppermute(over, 'dp', [(i, i ^ 2) for i in range(4)]))
    de = zero(de, FILLS[5], FILLS[6])
    y, dg, over, de = pl.pallas_call(
        final_kernel,
        out_shape=(jax.ShapeDtypeStruct((span, hidden), BF16), jax.ShapeDtypeStruct((1, hidden), F32),
                   jax.ShapeDtypeStruct((1, 1), jnp.int32), de_shape),
        in_specs=[VMEM] * 12 + [ANY], out_specs=(VMEM, VMEM, VMEM, ANY), input_output_aliases={12: 3},
        scratch_shapes=[pltpu.SMEM((8, 256), jnp.int32), pltpu.VMEM((U_CAP, SLAB, hidden), F32), pltpu.VMEM((span, hidden), F32),
                        pltpu.VMEM((span, 128), F32), pltpu.VMEM((1, hidden), F32), zeros, pltpu.SemaphoreType.DMA((3,))],
        compiler_params=pltpu.CompilerParams(vmem_limit_bytes=32 << 20),
        cost_estimate=cost(5, 8 << 20), name='final')(lst, over, idx, sums, part, u_got, u_fwd, norm_gain, *dgs, de)

    def keep(y, de, dg):
        return y, de, dg

    def redo(y, de, dg):
        y, de, dg = dense_step(token_ids, table_block, norm_gain, grad_block)
        return y, de.reshape(slabs, SLAB, hidden), dg.reshape(1, hidden)

    y, de, dg = lax.cond(over.reshape(()) > 0, redo, keep, y, de, dg)
    return y[None], de.reshape(rows, hidden), dg.reshape(hidden)


def solution(mesh):
    return jax.shard_map(device_step, mesh=mesh, in_specs=(P('dp', None), P('tp', None), P(None), P('dp', 'tp', None)), out_specs=(P('dp', 'tp', None), P(('dp', 'tp'), None), P('dp')), check_vma=False)
```
